32 devices in a mesh: dp: 1, expert: 32 (over z, y, x, core).
Axes of the slice: x: 2, y: 2, z: 4, core: 2. Of those that a mesh axis runs over, the one named last changes fastest.
Arguments:
- tokens: bfloat16 [8192, 2048], P(('dp', 'expert')), may hold values from -6 to 6
- expert_ranks: int32 [32, 8192], P(None, ('dp', 'expert')), may hold values from 0 to 8191, as said below
- capacity: int32 [32], replicated, may hold values from 64 to 128, as said below
- weight_in: bfloat16 [32, 2048, 8192], P('expert', None, 'dp'), may hold values from -0.125 to 0.125
- weight_out: bfloat16 [32, 8192, 2048], P('expert', 'dp'), may hold values from -0.0625 to 0.0625
- gate_weights: float32 [32, 128], P('expert', 'dp'), may hold values from 0.05 to 1
Outputs:
- combined: bfloat16 [8192, 2048], P(('dp', 'expert'))
The draws below stay inside these ranges and needn't reach their ends.
Inputs may be any that keep to these rules, and one draw needn't show every extreme that they name: `expert_ranks`: for each expert the ranks are a permutation of 0 to 8191. Of the 256 tokens of one device, at most 8 have rank under 128 for one expert; for an expert of capacity 128, some devices have exactly 8. At least one expert has capacity 128.
All inputs are finite; a program needn't handle non-finite values.
Results may differ from the reference program's by a relative error of at most 0.0053.
Values may be sent and summed in bfloat16 or wider, within the bound.
A program may use at most 128 MiB of HBM per device.

```python
import math
import jax
import jax.numpy as jnp
from jax import lax

D = 2048
FF = 8192
TOK_DEV = 256
EXPERTS = 32
TOKENS = 8192
CAP = 128


def local_permutation(subkey):
    return jax.random.permutation(subkey, TOK_DEV)


def device_permutation(subkey):
    return jax.random.permutation(subkey, TOKENS // TOK_DEV)


def token_permutation(subkey):
    return jax.random.permutation(subkey, TOKENS)


def draw_expert_ranks(key, part):
    devices_all = TOKENS // TOK_DEV
    average = TOK_DEV // 64
    low_total = 3 * average // 2
    key_mid = jax.random.fold_in(key, 11)
    key_low = jax.random.fold_in(key, 12)
    key_order = jax.random.fold_in(key, 13)
    key_local = jax.random.fold_in(key, 14)
    key_ties = jax.random.fold_in(key, 15)
    position = lax.broadcasted_iota(jnp.int32, (EXPERTS, devices_all), 1)
    paired = position // 2
    leading = position % 2 == 0
    middle_draw = jax.random.randint(key_mid, (EXPERTS, devices_all // 2), average // 2, average + average // 2 + 1)
    low_draw = jax.random.randint(key_low, (EXPERTS, devices_all // 2), average // 4, low_total - average // 4 + 1)
    middle_pick = jnp.take_along_axis(middle_draw, paired, axis=1)
    low_pick = jnp.take_along_axis(low_draw, paired, axis=1)
    middle_value = jnp.where(leading, middle_pick, 2 * average - middle_pick)
    low_value = jnp.where(leading, low_pick, low_total - low_pick)
    pattern = jnp.where(position < devices_all // 8, 2 * average, jnp.where(position < devices_all // 2, middle_value, low_value))
    orders = jax.vmap(device_permutation)(jax.random.split(key_order, EXPERTS))
    quota = jnp.take_along_axis(pattern, orders, axis=1).astype(jnp.int32)
    locals_all = jax.vmap(local_permutation)(jax.random.split(key_local, EXPERTS * devices_all))
    locals_all = locals_all.reshape(EXPERTS, devices_all, TOK_DEV)
    selected = (locals_all < quota[:, :, None]).reshape(EXPERTS, TOKENS)
    ties = jax.vmap(token_permutation)(jax.random.split(key_ties, EXPERTS)).astype(jnp.int32)
    score = jnp.where(selected, ties, TOKENS + ties).astype(jnp.int32)
    order = jnp.argsort(score, axis=1, stable=True)
    ranks = jnp.argsort(order, axis=1, stable=True)
    return ranks.astype(jnp.int32)


def draw_capacity(key, part):
    key_values = jax.random.fold_in(key, 21)
    key_full = jax.random.fold_in(key, 22)
    values = jax.random.randint(key_values, (EXPERTS,), CAP // 2, CAP + 1)
    full_index = jax.random.randint(key_full, (), 0, EXPERTS)
    position = lax.broadcasted_iota(jnp.int32, (EXPERTS,), 0)
    return jnp.where(position == full_index, CAP, values).astype(jnp.int32)


def shard_levels(key, shape, cuts, smallest, top_value):
    loudness = 1.0
    for axis_at, parts in cuts:
        steps = jax.random.uniform(jax.random.fold_in(jax.random.fold_in(key, 6), axis_at), (parts,), jnp.float32, smallest / len(cuts), top_value / len(cuts))
        loudness = loudness * jnp.repeat(jnp.exp(steps), shape[axis_at] // parts).reshape((-1,) + (1,) * (len(shape) - 1 - axis_at))
    return loudness


def gaussian(stream_key, shape, width, most, cuts=(), kind=jnp.bfloat16):
    result = jax.random.normal(stream_key, shape, jnp.float32) * width
    if len(cuts) > 0:
        result = shard_levels(stream_key, shape, cuts, -0.22, 0.18) * result
    return jnp.clip(result, min=-most, max=most).astype(kind)


def setup_inputs(seed: int = 0) -> dict:
    key_list = jax.random.split(jax.random.key(seed), 7)
    tokens = gaussian(key_list[0], (TOKENS, D), 1.0, 6.0, ((0, 32),))
    expert_ranks = draw_expert_ranks(jax.random.fold_in(key_list[6], 71), 0)
    capacity = draw_capacity(jax.random.fold_in(key_list[6], 71), 0)
    weight_in = gaussian(key_list[3], (EXPERTS, D, FF), D ** -0.5, 0.125, ((0, 32),))
    weight_out = gaussian(key_list[4], (EXPERTS, FF, D), FF ** -0.5, 0.0625, ((0, 32),))
    gate_weights = jnp.clip(jnp.exp(math.log(1.0) - 2.9957323 * jax.random.uniform(key_list[5], (EXPERTS, CAP), jnp.float32) ** shard_levels(key_list[5], (EXPERTS, CAP), ((0, 32),), -0.2, 0.2)), 0.05, 1.0)
    return {"tokens": tokens, "expert_ranks": expert_ranks, "capacity": capacity, "weight_in": weight_in, "weight_out": weight_out, "gate_weights": gate_weights}


def reference(tokens, expert_ranks, capacity, weight_in, weight_out, gate_weights):
    total = tokens.shape[0]
    tokens_wide = tokens.astype(jnp.float32)

    def one_expert(accum, index):
        rank_row = lax.dynamic_index_in_dim(expert_ranks, index, 0, keepdims=False)
        limit = lax.dynamic_index_in_dim(capacity, index, 0, keepdims=False)
        chosen = rank_row < limit
        chosen_int = chosen.astype(jnp.int32)
        slots = (jnp.cumsum(chosen_int).astype(jnp.int32) - chosen_int).astype(jnp.int32)
        target = jnp.where(chosen, slots, CAP).astype(jnp.int32)
        slot_rows = jnp.zeros((CAP + 1, D), jnp.float32).at[target].add(tokens_wide)[:CAP].astype(jnp.bfloat16)
        first_weight = lax.dynamic_index_in_dim(weight_in, index, 0, keepdims=False)
        second_weight = lax.dynamic_index_in_dim(weight_out, index, 0, keepdims=False)
        hidden = jnp.maximum(jnp.dot(slot_rows, first_weight, preferred_element_type=jnp.float32), 0.0).astype(jnp.bfloat16)
        expert_out = jnp.dot(hidden, second_weight, preferred_element_type=jnp.float32)
        gates = lax.dynamic_index_in_dim(gate_weights, index, 0, keepdims=False)
        scaled = (gates[:, None] * expert_out).astype(jnp.bfloat16)
        picked = jnp.take(scaled, jnp.minimum(slots, CAP - 1).astype(jnp.int32), axis=0)
        accum = accum + jnp.where(chosen[:, None], picked.astype(jnp.float32), 0.0)
        return accum, None

    accum, unused = lax.scan(one_expert, jnp.zeros((total, D), jnp.float32), jnp.arange(EXPERTS, dtype=jnp.int32))
    return accum.astype(jnp.bfloat16)
```

```python
import jax
import jax.numpy as jnp
from jax import lax
from jax.experimental import pallas as pl
from jax.experimental.pallas import tpu as pltpu
from jax.sharding import PartitionSpec as P

MOST = 8
PAIR = 2 * MOST
CHUNKS = 2
SLOTS_PER_CHUNK = 3
MESH = pl.DeviceIdType.MESH


def one_hot(condition):
    return jnp.where(condition, 1.0, 0.0)


def fused(
    tokens, ranks, capacity, gates, weight_in, weight_out, combined,
    wbuf, send_rows, got_rows, send_back, got_back, acc, hidden, oacc, take_left, take_right,
    wsem, send_sem, recv_sem, own_sem,
):
    n = lax.axis_size("expert")
    me = lax.axis_index("expert")
    dp = lax.axis_index("dp")
    token_count, width = tokens.shape
    slots = gates.shape[1]
    rows = n * PAIR
    half = width // 2
    part = half // CHUNKS
    nslots, blocks = wbuf.shape[0], wbuf.shape[1]
    first_units = 2 * CHUNKS
    units = 4 * CHUNKS

    def load_unit(u):
        slot = u % nslots
        which = u % first_units
        offset = (which % 2) * half + (which // 2) * part

        def start(j, carry):
            at = pl.multiple_of(j * part, part)
            if u < first_units:
                src = weight_in.at[0, pl.ds(offset, part), pl.ds(at, part)]
            else:
                src = weight_out.at[0, pl.ds(at, part), pl.ds(offset, part)]
            pltpu.make_async_copy(src, wbuf.at[slot, j], wsem.at[u]).start()
            return carry

        lax.fori_loop(0, blocks, start, 0)

    def wait_unit(u):
        slot = u % nslots
        pltpu.make_async_copy(wbuf.at[slot], wbuf.at[slot], wsem.at[u]).wait()

    barrier = pltpu.get_barrier_semaphore()

    def greet(k, carry):
        peer = lax.rem(me + k, n)
        pl.semaphore_signal(barrier, inc=1, device_id=(dp, peer), device_id_type=MESH)
        return carry

    lax.fori_loop(1, n, greet, 0)
    for u in range(nslots):
        load_unit(u)

    def columns(c, extra):
        if extra == 0:
            return pl.ds(c * part, part)
        return pl.ds(0, extra + part) if c == 0 else pl.ds(extra + c * part, part)

    def exchange(src, dst, phase, c, extra):
        cols = columns(c, extra)
        index = phase * CHUNKS + c

        def send(k, carry):
            peer = lax.rem(me + k, n)
            pltpu.make_async_remote_copy(
                src_ref=src.at[pl.ds(pl.multiple_of(peer * PAIR, PAIR), PAIR), cols],
                dst_ref=dst.at[pl.ds(pl.multiple_of(me * PAIR, PAIR), PAIR), cols],
                send_sem=send_sem.at[index],
                recv_sem=recv_sem.at[index],
                device_id=(dp, peer),
                device_id_type=MESH,
            ).start()
            return carry

        lax.fori_loop(1, n, send, 0)
        mine = pl.ds(pl.multiple_of(me * PAIR, PAIR), PAIR)
        pltpu.make_async_copy(src.at[mine, cols], dst.at[mine, cols], own_sem.at[index]).start()

    def arrive(src, dst, phase, c, extra):
        cols = columns(c, extra)
        index = phase * CHUNKS + c
        mine = pl.ds(pl.multiple_of(me * PAIR, PAIR), PAIR)
        pltpu.make_async_copy(src.at[mine, cols], dst.at[mine, cols], own_sem.at[index]).wait()
        most = dst.at[pl.ds(0, (n - 1) * PAIR), cols]
        pltpu.make_async_copy(most, most, recv_sem.at[index]).wait()

    def left(src, phase, c, extra):
        most = src.at[pl.ds(0, (n - 1) * PAIR), columns(c, extra)]
        index = phase * CHUNKS + c
        pltpu.make_async_copy(most, most, send_sem.at[index]).wait()

    chosen = ranks[...] < capacity[...]
    chosen_one = one_hot(chosen)
    t_from = lax.broadcasted_iota(jnp.int32, (token_count, token_count), 0)
    t_to = lax.broadcasted_iota(jnp.int32, (token_count, token_count), 1)
    earlier = one_hot(t_from < t_to).astype(jnp.bfloat16)
    before = jnp.dot(chosen_one.astype(jnp.bfloat16), earlier, preferred_element_type=jnp.float32)
    code = jnp.where(chosen, jnp.minimum(before, float(MOST)), float(MOST)).astype(jnp.bfloat16)
    row_of = lax.broadcasted_iota(jnp.int32, (rows, n), 0)
    expert_of = lax.broadcasted_iota(jnp.int32, (rows, n), 1)
    first_row = expert_of * PAIR
    repeat = one_hot(jnp.logical_and(row_of >= first_row, row_of < first_row + PAIR))
    code_rows = jnp.dot(repeat.astype(jnp.bfloat16), code, preferred_element_type=jnp.float32)
    row_id = lax.broadcasted_iota(jnp.int32, (rows, token_count), 0)
    place = jnp.bitwise_and(row_id, MOST - 1).astype(jnp.float32)
    on_right = jnp.bitwise_and(row_id, MOST) > 0
    hit = one_hot(code_rows == place)
    pick_left = jnp.where(on_right, 0.0, hit)
    pick_right = jnp.where(on_right, hit, 0.0)
    ones = jnp.ones((token_count, slots), jnp.bfloat16)
    send_rows[:, pl.ds(0, slots)] = jnp.dot(
        hit.astype(jnp.bfloat16), ones, preferred_element_type=jnp.float32
    ).astype(jnp.bfloat16)
    pick_left_low = pick_left.astype(jnp.bfloat16)
    pick_right_low = pick_right.astype(jnp.bfloat16)
    for c in range(CHUNKS):
        send_rows[:, pl.ds(slots + c * part, part)] = (
            jnp.dot(
                pick_left_low, tokens[:, pl.ds(c * part, part)],
                preferred_element_type=jnp.float32,
            )
            + jnp.dot(
                pick_right_low, tokens[:, pl.ds(half + c * part, part)],
                preferred_element_type=jnp.float32,
            )
        ).astype(jnp.bfloat16)
        if c == 0:
            pl.semaphore_wait(barrier, n - 1)
        exchange(send_rows, got_rows, 0, c, slots)
    take_left[...] = pick_left.T.astype(jnp.bfloat16)
    take_right[...] = pick_right.T.astype(jnp.bfloat16)
    gate_column = jnp.broadcast_to(gates[...], (slots, slots)).T[:, 0:1]
    r_to = lax.broadcasted_iota(jnp.int32, (rows, rows), 0)
    r_from = lax.broadcasted_iota(jnp.int32, (rows, rows), 1)
    base = r_to - jnp.bitwise_and(r_to, MOST)
    ahead = one_hot(jnp.logical_and(r_from < base, jnp.bitwise_and(r_from, MOST) == 0))
    ahead = ahead.astype(jnp.bfloat16)

    arrive(send_rows, got_rows, 0, 0, slots)
    valid = got_rows[:, pl.ds(0, slots)]
    slot_of = jnp.dot(ahead, valid, preferred_element_type=jnp.float32)
    slot_id = lax.broadcasted_iota(jnp.int32, (rows, slots), 1).astype(jnp.float32)
    spot = jnp.where(slot_of == slot_id, valid.astype(jnp.float32), 0.0)
    right_row = jnp.bitwise_and(lax.broadcasted_iota(jnp.int32, (rows, slots), 0), MOST) > 0
    put_left = jnp.where(right_row, 0.0, spot)
    put_right = jnp.where(right_row, spot, 0.0)
    get_left = put_left.T.astype(jnp.bfloat16)
    get_right = put_right.T.astype(jnp.bfloat16)
    put_left = put_left.astype(jnp.bfloat16)
    put_right = put_right.astype(jnp.bfloat16)

    for c in range(CHUNKS):
        if c > 0:
            arrive(send_rows, got_rows, 0, c, slots)
        here = got_rows[:, pl.ds(slots + c * part, part)]
        x_left = jnp.dot(get_left, here, preferred_element_type=jnp.float32).astype(jnp.bfloat16)
        x_right = jnp.dot(get_right, here, preferred_element_type=jnp.float32).astype(jnp.bfloat16)
        u = 2 * c
        wait_unit(u)
        wait_unit(u + 1)

        def first(j, carry):
            term = jnp.dot(x_left, wbuf[u % nslots, j], preferred_element_type=jnp.float32)
            term += jnp.dot(x_right, wbuf[(u + 1) % nslots, j], preferred_element_type=jnp.float32)
            if c > 0:
                term += acc[j]
            if c < CHUNKS - 1:
                acc[j] = term
            else:
                hidden[j] = jnp.maximum(term, 0.0).astype(jnp.bfloat16)
            return carry

        lax.fori_loop(0, blocks, first, 0)
        for v in (u, u + 1):
            if v + nslots < units:
                load_unit(v + nslots)

    for c in range(CHUNKS):
        u = first_units + 2 * c
        wait_unit(u)
        wait_unit(u + 1)
        oacc[...] = jnp.zeros_like(oacc)

        def second(j, carry):
            for side in range(2):
                term = oacc[side]
                for i in range(2):
                    term += jnp.dot(
                        hidden[2 * j + i], wbuf[(u + side) % nslots, 2 * j + i],
                        preferred_element_type=jnp.float32,
                    )
                oacc[side] = term
            return carry

        lax.fori_loop(0, blocks // 2, second, 0)
        scaled_left = (gate_column * oacc[0]).astype(jnp.bfloat16)
        scaled_right = (gate_column * oacc[1]).astype(jnp.bfloat16)
        send_back[:, pl.ds(c * part, part)] = (
            jnp.dot(put_left, scaled_left, preferred_element_type=jnp.float32)
            + jnp.dot(put_right, scaled_right, preferred_element_type=jnp.float32)
        ).astype(jnp.bfloat16)
        for v in (u, u + 1):
            if v + nslots < units:
                load_unit(v + nslots)
        exchange(send_back, got_back, 1, c, 0)

    for c in range(CHUNKS):
        arrive(send_back, got_back, 1, c, 0)
        here = got_back[:, pl.ds(c * part, part)]
        combined[:, pl.ds(c * part, part)] = jnp.dot(
            take_left[...], here, preferred_element_type=jnp.float32
        ).astype(combined.dtype)
        combined[:, pl.ds(half + c * part, part)] = jnp.dot(
            take_right[...], here, preferred_element_type=jnp.float32
        ).astype(combined.dtype)
    for c in range(CHUNKS):
        left(send_rows, 0, c, slots)
        left(send_back, 1, c, 0)


def on_device_fused(tokens, expert_ranks, capacity, weight_in, weight_out, gate_weights):
    n = lax.axis_size("expert")
    token_count, width = tokens.shape
    hidden_units = weight_in.shape[2]
    slots = gate_weights.shape[1]
    rows = n * PAIR
    half = width // 2
    part = half // CHUNKS
    blocks = hidden_units // part
    low, wide = jnp.bfloat16, jnp.float32
    vmem = pl.BlockSpec(memory_space=pltpu.VMEM)
    anywhere = pl.BlockSpec(memory_space=pl.ANY)
    return pl.pallas_call(
        fused,
        out_shape=jax.ShapeDtypeStruct((token_count, width), low),
        in_specs=[vmem, vmem, vmem, vmem, anywhere, anywhere],
        out_specs=vmem,
        scratch_shapes=[
            pltpu.VMEM((SLOTS_PER_CHUNK * CHUNKS, blocks, part, part), low),
            pltpu.VMEM((rows, slots + half), low),
            pltpu.VMEM((rows, slots + half), low),
            pltpu.VMEM((rows, half), low),
            pltpu.VMEM((rows, half), low),
            pltpu.VMEM((blocks, slots, part), wide),
            pltpu.VMEM((blocks, slots, part), low),
            pltpu.VMEM((2, slots, part), wide),
            pltpu.VMEM((token_count, rows), low),
            pltpu.VMEM((token_count, rows), low),
            pltpu.SemaphoreType.DMA((4 * CHUNKS,)),
            pltpu.SemaphoreType.DMA((2 * CHUNKS,)),
            pltpu.SemaphoreType.DMA((2 * CHUNKS,)),
            pltpu.SemaphoreType.DMA((2 * CHUNKS,)),
        ],
        compiler_params=pltpu.CompilerParams(
            collective_id=0, has_side_effects=True, vmem_limit_bytes=67043328
        ),
        name="fused",
    )(tokens, expert_ranks, capacity[:, None], gate_weights, weight_in, weight_out)


def on_device(tokens, expert_ranks, capacity, weight_in, weight_out, gate_weights):
    dp_count = lax.axis_size("dp")
    expert_count = lax.axis_size("expert")
    token_count, width = tokens.shape
    slots_all = gate_weights.shape[1] * dp_count
    chosen = expert_ranks < capacity[:, None]
    chosen_int = chosen.astype(jnp.int32)
    counts = jnp.sum(chosen_int, axis=1)
    before = jnp.cumsum(chosen_int, axis=1) - chosen_int
    places = lax.broadcasted_iota(jnp.int32, (expert_count, MOST, token_count), 1)
    pack_table = jnp.logical_and(chosen[:, None, :], before[:, None, :] == places)
    pack_table = pack_table.astype(jnp.bfloat16).reshape(expert_count * MOST, token_count)
    packed = jnp.dot(pack_table, tokens, preferred_element_type=jnp.float32).astype(jnp.bfloat16)
    arrived_rows = lax.all_to_all(
        packed.reshape(expert_count, MOST, width), "expert", split_axis=0, concat_axis=0, tiled=True
    )
    own_expert = lax.axis_index("expert")
    expert_mask = (lax.broadcasted_iota(jnp.int32, (expert_count,), 0) == own_expert).astype(
        jnp.int32
    )
    count_table = lax.all_gather(counts[None, :], ("dp", "expert"), axis=0, tiled=True)
    column = jnp.sum(count_table * expert_mask[None, :], axis=1)
    earlier_sums = jnp.cumsum(column) - column
    row_first = lax.axis_index("dp") * expert_count
    starts = lax.dynamic_slice_in_dim(earlier_sums, row_first, expert_count, 0)
    arrived = lax.dynamic_slice_in_dim(column, row_first, expert_count, 0)
    within = lax.broadcasted_iota(jnp.int32, (expert_count, MOST), 1)
    target = jnp.where(within < arrived[:, None], starts[:, None] + within, -1).reshape(
        expert_count * MOST
    )
    slot_ids = lax.broadcasted_iota(jnp.int32, (expert_count * MOST, slots_all), 1)
    place_table = (target[:, None] == slot_ids).astype(jnp.bfloat16)
    flat_rows = arrived_rows.reshape(expert_count * MOST, width)
    local_rows = lax.dot_general(
        place_table, flat_rows, (((0,), (0,)), ((), ())), preferred_element_type=jnp.float32
    ).astype(jnp.bfloat16)
    first_weight = weight_in[0]
    second_weight = weight_out[0]
    slot_rows = lax.psum(local_rows, "dp").astype(jnp.float32).astype(jnp.bfloat16)
    hidden = jnp.maximum(
        jnp.dot(slot_rows, first_weight, preferred_element_type=jnp.float32), 0.0
    ).astype(jnp.bfloat16)
    out_share = lax.psum_scatter(
        jnp.dot(hidden, second_weight, preferred_element_type=jnp.float32),
        "dp",
        scatter_dimension=0,
        tiled=True,
    )
    scaled = (gate_weights[0][:, None] * out_share).astype(jnp.bfloat16)
    returned = jnp.dot(
        place_table,
        lax.all_gather(scaled, "dp", axis=0, tiled=True),
        preferred_element_type=jnp.float32,
    )
    sent_back = returned.astype(jnp.bfloat16).reshape(expert_count, MOST, width)
    results = lax.all_to_all(sent_back, "expert", split_axis=0, concat_axis=0, tiled=True)
    flat_results = results.reshape(expert_count * MOST, width)
    combined = lax.dot_general(
        pack_table, flat_results, (((0,), (0,)), ((), ())), preferred_element_type=jnp.float32
    )
    return combined.astype(jnp.bfloat16)


def solution(mesh):
    in_specs = (
        P(("dp", "expert"), None),
        P(None, ("dp", "expert")),
        P(),
        P("expert", None, "dp"),
        P("expert", "dp", None),
        P("expert", "dp"),
    )
    out_specs = P(("dp", "expert"), None)
    one_share = mesh.shape["dp"] == 1
    return jax.shard_map(
        on_device_fused if one_share else on_device, mesh=mesh, in_specs=in_specs, out_specs=out_specs, check_vma=False
    )
```
